8 devices in a mesh: data: 8 (over z, y, x, core).
Axes of the slice: x: 2, y: 2, z: 1, core: 2. Of those that a mesh axis runs over, the one named last changes fastest.
Arguments:
- x_now: bfloat16 [32, 577, 1024], P('data')
- x_next: bfloat16 [32, 577, 1024], P('data')
- labels: int32 [32], P('data')
- w_up: float32 [6, 1024, 4096], replicated
- w_down: float32 [6, 4096, 1024], replicated
- w_head: float32 [1024, 1000], replicated
- mom_up: float32 [6, 1024, 4096], P(None, None, 'data')
- mom_down: float32 [6, 4096, 1024], P(None, 'data')
- mom_head: float32 [1024, 1000], P('data')
- learn_rate: float32 [], replicated
- mom_decay: float32 [], replicated
Outputs:
- output 1: float32 [32, 1000], P('data')
- output 2: float32 [6, 1024, 4096], replicated
- output 3: float32 [6, 4096, 1024], replicated
- output 4: float32 [1024, 1000], replicated
- output 5: float32 [6, 1024, 4096], P(None, None, 'data')
- output 6: float32 [6, 4096, 1024], P(None, 'data')
- output 7: float32 [1024, 1000], P('data')
All inputs are finite; a program needn't handle non-finite values.
Results may differ from the reference program's by a relative error of at most 0.011512.
Values are sent between devices in bfloat16 or wider.
A program may use at most 2 GiB of HBM per device.

```python
import math
import jax
import jax.numpy as jnp
from jax import lax

BATCH_DEV = 4
TOKENS = 577
WIDTH = 1024
HIDDEN = 4096
CLASSES = 1000
LAYERS = 6
GROUPS = 8
LN_EPS = 1e-6


def setup_inputs(seed: int = 0) -> dict:
    keys = jax.random.split(jax.random.key(seed), 13)
    batch = GROUPS * BATCH_DEV
    mom_scale = batch ** -0.5
    img_now = jax.random.normal(keys[0], (batch, 1, WIDTH), jnp.float32)
    tok_now = jax.random.normal(keys[1], (batch, TOKENS, WIDTH), jnp.float32)
    img_next = jax.random.normal(keys[2], (batch, 1, WIDTH), jnp.float32)
    tok_next = jax.random.normal(keys[3], (batch, TOKENS, WIDTH), jnp.float32)
    down_raw = jax.random.normal(keys[6], (LAYERS, HIDDEN, WIDTH), jnp.float32) * HIDDEN ** -0.5
    mom_raw = jax.random.normal(keys[9], (LAYERS, HIDDEN, WIDTH), jnp.float32) * (HIDDEN ** -0.5 * mom_scale)
    return {
        "x_now": (0.8 * img_now + 0.6 * tok_now).astype(jnp.bfloat16),
        "x_next": (0.8 * img_next + 0.6 * tok_next).astype(jnp.bfloat16),
        "labels": jax.random.randint(keys[4], (batch,), 0, CLASSES, jnp.int32),
        "w_up": jax.random.normal(keys[5], (LAYERS, WIDTH, HIDDEN), jnp.float32) * WIDTH ** -0.5,
        "w_down": down_raw - jnp.mean(down_raw, axis=1, keepdims=True),
        "w_head": jax.random.normal(keys[7], (WIDTH, CLASSES), jnp.float32) * WIDTH ** -0.5,
        "mom_up": jax.random.normal(keys[8], (LAYERS, WIDTH, HIDDEN), jnp.float32) * (WIDTH ** -0.5 * mom_scale),
        "mom_down": mom_raw - jnp.mean(mom_raw, axis=1, keepdims=True),
        "mom_head": jax.random.normal(keys[10], (WIDTH, CLASSES), jnp.float32) * (WIDTH ** -0.5 * mom_scale),
        "learn_rate": jax.random.uniform(keys[11], (), jnp.float32, 0.3, 0.6) * math.sqrt(batch),
        "mom_decay": jax.random.uniform(keys[12], (), jnp.float32, 0.7, 0.95),
    }


def norm_rows(values):
    mean_v = jnp.mean(values, axis=-1, keepdims=True)
    centered = values - mean_v
    var_v = jnp.mean(centered * centered, axis=-1, keepdims=True)
    return centered * lax.rsqrt(var_v + LN_EPS)


def block_fwd(x_rows, w_in, w_out):
    x_wide = x_rows.astype(jnp.float32)
    u_rows = norm_rows(x_wide).astype(jnp.bfloat16)
    pre_act = jnp.dot(u_rows, w_in.astype(jnp.bfloat16), preferred_element_type=jnp.float32).astype(jnp.bfloat16)
    gelu_out = jax.nn.gelu(pre_act.astype(jnp.float32), approximate=True).astype(jnp.bfloat16)
    block_out = jnp.dot(gelu_out, w_out.astype(jnp.bfloat16), preferred_element_type=jnp.float32).astype(jnp.bfloat16)
    return (x_wide + block_out.astype(jnp.float32)).astype(jnp.bfloat16)


def group_logits(x_grp, w_up, w_down, w_head):
    n_img, n_tok, width = x_grp.shape

    def layer_step(rows, layer_w):
        return block_fwd(rows, layer_w[0], layer_w[1]), None

    rows, _ = lax.scan(layer_step, x_grp.reshape(n_img * n_tok, width), (w_up, w_down))
    pooled = jnp.mean(rows.reshape(n_img, n_tok, width), axis=1, dtype=jnp.float32)
    normed = norm_rows(pooled).astype(jnp.bfloat16)
    return jnp.dot(normed, w_head.astype(jnp.bfloat16), preferred_element_type=jnp.float32)


def cross_ent(logits, labels):
    log_norm = jax.nn.logsumexp(logits, axis=-1)
    picked = jnp.sum(logits * jax.nn.one_hot(labels, logits.shape[-1], dtype=logits.dtype), axis=-1)
    return log_norm - picked


def reference(x_now, x_next, labels, w_up, w_down, w_head, mom_up, mom_down, mom_head, learn_rate, mom_decay):
    weights = (w_up, w_down, w_head)
    batch_total = GROUPS * BATCH_DEV
    x_groups = x_now.reshape(GROUPS, BATCH_DEV, TOKENS, WIDTH)
    label_groups = labels.reshape(GROUPS, BATCH_DEV)

    def accumulate(total, group):
        x_grp, lab_grp = group

        def group_loss(params):
            logits = group_logits(x_grp, params[0], params[1], params[2])
            return jnp.sum(cross_ent(logits, lab_grp)) / batch_total

        _, loss_pull = jax.vjp(group_loss, weights)
        gradients = loss_pull(jnp.ones((), jnp.float32))[0]
        return (total[0] + gradients[0], total[1] + gradients[1], total[2] + gradients[2]), None

    zero_grads = (jnp.zeros_like(w_up), jnp.zeros_like(w_down), jnp.zeros_like(w_head))
    gradients, _ = lax.scan(accumulate, zero_grads, (x_groups, label_groups))
    new_mom_up = mom_decay * mom_up + gradients[0]
    new_mom_down = mom_decay * mom_down + gradients[1]
    new_mom_head = mom_decay * mom_head + gradients[2]
    new_w_up = w_up - learn_rate * new_mom_up
    new_w_down = w_down - learn_rate * new_mom_down
    new_w_head = w_head - learn_rate * new_mom_head
    next_groups = x_next.reshape(GROUPS, BATCH_DEV, TOKENS, WIDTH)
    logits_next = lax.map(lambda x_grp: group_logits(x_grp, new_w_up, new_w_down, new_w_head), next_groups)
    logits_next = logits_next.reshape(GROUPS * BATCH_DEV, CLASSES)
    return (logits_next, new_w_up, new_w_down, new_w_head, new_mom_up, new_mom_down, new_mom_head)
```

```python
import functools

import jax
import jax.numpy as jnp
from jax import lax
from jax.experimental import pallas as pl
from jax.experimental.pallas import tpu as pltpu
from jax.sharding import PartitionSpec as P


LN_EPS = 1e-6
GELU_A = 0.7978845608028654
GELU_B = GELU_A * 0.044715
BF = jnp.bfloat16
F32 = jnp.float32
CONTRACT_ROWS = (((0,), (0,)), ((), ()))
CONTRACT_LAST = (((1,), (1,)), ((), ()))
ONCE = pl.Buffered(1)
ROW_BLOCKS = 5
EARLY = 3


def norm_rows(values):
    mean_v = jnp.mean(values, axis=-1, keepdims=True)
    centered = values - mean_v
    var_v = jnp.mean(centered * centered, axis=-1, keepdims=True)
    return centered * lax.rsqrt(var_v + LN_EPS)


def gelu_tanh(a):
    t = jnp.tanh(a * (GELU_A + GELU_B * (a * a)))
    return a * (0.5 + 0.5 * t)


def row_slice(r, size):
    return pl.ds(pl.multiple_of(r * size, 16), size)


def fwd_now_body(x_ref, wu_ref, wd_ref, a_ref, xo_ref, x_s, u_s, acc_s):
    layer, c = pl.program_id(0), pl.program_id(1)
    last = pl.num_programs(1) - 1
    rb = x_s.shape[0] // ROW_BLOCKS

    @pl.when((layer == 0) & (c == 0))
    def _():
        @pl.loop(0, ROW_BLOCKS)
        def _(r):
            rs = row_slice(r, rb)
            x = x_ref[rs, :]
            x_s[rs, :] = x
            u_s[rs, :] = norm_rows(x.astype(F32)).astype(BF)
            acc_s[rs, :] = jnp.zeros((rb, x.shape[1]), F32)

    wu = wu_ref[...].astype(BF)
    wd = wd_ref[...].astype(BF)

    def up(r):
        rs = pl.ds(r * rb, rb)
        a = jnp.dot(u_s[rs, :], wu, preferred_element_type=F32).astype(BF)
        a_ref[rs, :] = a
        return gelu_tanh(a.astype(F32)).astype(BF)

    z = up(0)
    for r in range(ROW_BLOCKS):
        z_next = up(r + 1) if r + 1 < ROW_BLOCKS else None
        acc_s[pl.ds(r * rb, rb), :] += jnp.dot(z, wd, preferred_element_type=F32)
        z = z_next

    @pl.when(c == last)
    def _():
        @pl.loop(0, ROW_BLOCKS)
        def _(r):
            rs = row_slice(r, rb)
            x = (x_s[rs, :].astype(F32) + acc_s[rs, :].astype(BF).astype(F32)).astype(BF)
            x_s[rs, :] = x
            xo_ref[rs, :] = x
            u_s[rs, :] = norm_rows(x.astype(F32)).astype(BF)
            acc_s[rs, :] = jnp.zeros((rb, x.shape[1]), F32)


def fwd_now(x, w_up, w_down, n_chunk):
    rows, width = x.shape
    layers, _, hidden = w_up.shape
    ch = hidden // n_chunk
    return pl.pallas_call(
        fwd_now_body,
        grid=(layers, n_chunk),
        in_specs=[
            pl.BlockSpec((rows, width), lambda l, c: (0, 0), pipeline_mode=ONCE),
            pl.BlockSpec((None, width, ch), lambda l, c: (l, 0, c)),
            pl.BlockSpec((None, ch, width), lambda l, c: (l, c, 0)),
        ],
        out_specs=[
            pl.BlockSpec((None, rows, ch), lambda l, c: (l, 0, c)),
            pl.BlockSpec((None, rows, width), lambda l, c: (l, 0, 0)),
        ],
        out_shape=[
            jax.ShapeDtypeStruct((layers, rows, hidden), BF),
            jax.ShapeDtypeStruct((layers, rows, width), BF),
        ],
        scratch_shapes=[
            pltpu.VMEM((rows, width), BF),
            pltpu.VMEM((rows, width), BF),
            pltpu.VMEM((rows, width), F32),
        ],
        compiler_params=pltpu.CompilerParams(
            vmem_limit_bytes=62 * 2**20, dimension_semantics=("arbitrary", "arbitrary")
        ),
        cost_estimate=pl.CostEstimate(
            flops=layers * 4 * rows * width * hidden,
            bytes_accessed=layers * (8 * width * hidden + 2 * rows * (width + hidden)),
            transcendentals=layers * rows * hidden,
        ),
        name="fwd_now",
    )(x, w_up, w_down)


def bwd_body(need_dx, g_ref, x_ref, a_ref, wu_ref, wd_ref, dw_ref, *rest):
    if need_dx:
        go_ref, u_s, z_s, dp_s, acc_s = rest
    else:
        u_s, z_s, dp_s = rest
    c = pl.program_id(0)
    last = pl.num_programs(0) - 1
    rb = u_s.shape[0] // ROW_BLOCKS
    width = u_s.shape[1]
    ch = z_s.shape[1]

    @pl.when(c == 0)
    def _():
        @pl.loop(0, ROW_BLOCKS)
        def _(r):
            rs = row_slice(r, rb)
            u_s[rs, :] = norm_rows(x_ref[rs, :].astype(F32)).astype(BF)
            if need_dx:
                acc_s[rs, :] = jnp.zeros((rb, width), F32)

    wd = wd_ref[...].astype(BF)
    wu = wu_ref[...].astype(BF) if need_dx else None

    def grad_pre(r):
        rs = pl.ds(r * rb, rb)
        dz = lax.dot_general(g_ref[rs, :], wd, CONTRACT_LAST, preferred_element_type=F32)
        dz = dz.astype(BF).astype(F32)
        a = a_ref[rs, :].astype(F32)
        a2 = a * a
        t = jnp.tanh(a * (GELU_A + GELU_B * a2))
        s = 0.5 + 0.5 * t
        z = a * s
        slope = s + (z * (0.5 - 0.5 * t)) * (2 * GELU_A + (6 * GELU_B) * a2)
        dp = (slope * dz).astype(BF)
        z_s[rs, :] = z.astype(BF)
        dp_s[rs, :] = dp
        return dp

    dp = grad_pre(0)
    for r in range(ROW_BLOCKS):
        dp_next = grad_pre(r + 1) if r + 1 < ROW_BLOCKS else None
        if need_dx:
            du = lax.dot_general(dp, wu, CONTRACT_LAST, preferred_element_type=F32)
            acc_s[pl.ds(r * rb, rb), :] += du
        dp = dp_next

    dwd = lax.dot_general(z_s[...], g_ref[...], CONTRACT_ROWS, preferred_element_type=F32)
    dwd = dwd.astype(BF)
    dwu = lax.dot_general(u_s[...], dp_s[...], CONTRACT_ROWS, preferred_element_type=F32)
    dw_ref[0:width, :] = dwu.astype(BF)
    for part in range(width // ch):
        dw_ref[width + part * ch:width + (part + 1) * ch, :] = dwd[:, part * ch:(part + 1) * ch]

    if need_dx:
        @pl.when(c == last)
        def _():
            @pl.loop(0, ROW_BLOCKS)
            def _(r):
                rs = row_slice(r, rb)
                xw = x_ref[rs, :].astype(F32)
                centered = xw - jnp.mean(xw, axis=-1, keepdims=True)
                var_v = jnp.mean(centered * centered, axis=-1, keepdims=True)
                rstd = lax.rsqrt(var_v + LN_EPS)
                xhat = centered * rstd
                du = acc_s[rs, :].astype(BF).astype(F32)
                m1 = jnp.mean(du, axis=-1, keepdims=True)
                m2 = jnp.mean(du * xhat, axis=-1, keepdims=True)
                dx = rstd * (du - m1 - xhat * m2)
                go_ref[rs, :] = (g_ref[rs, :].astype(F32) + dx).astype(BF)


def bwd_block(g, x, x_index, a, w_up, w_down, layer, n_chunk):
    rows, width = g.shape
    hidden = w_up.shape[2]
    ch = hidden // n_chunk
    need_dx = layer > 0
    if x.ndim == 3:
        x_spec = pl.BlockSpec((None, rows, width), lambda c: (x_index, 0, 0), pipeline_mode=ONCE)
    else:
        x_spec = pl.BlockSpec((rows, width), lambda c: (0, 0), pipeline_mode=ONCE)
    dw_rows = 2 * width
    out_specs = [pl.BlockSpec((None, dw_rows, ch), lambda c: (c, 0, 0))]
    out_shape = [jax.ShapeDtypeStruct((n_chunk, dw_rows, ch), BF)]
    scratch = [pltpu.VMEM((rows, width), BF), pltpu.VMEM((rows, ch), BF), pltpu.VMEM((rows, ch), BF)]
    if need_dx:
        out_specs.append(pl.BlockSpec((rows, width), lambda c: (0, 0), pipeline_mode=ONCE))
        out_shape.append(jax.ShapeDtypeStruct((rows, width), BF))
        scratch.append(pltpu.VMEM((rows, width), F32))
    return pl.pallas_call(
        functools.partial(bwd_body, need_dx),
        grid=(n_chunk,),
        in_specs=[
            pl.BlockSpec((rows, width), lambda c: (0, 0), pipeline_mode=ONCE),
            x_spec,
            pl.BlockSpec((None, rows, ch), lambda c: (layer, 0, c)),
            pl.BlockSpec((None, width, ch), lambda c: (layer, 0, c)),
            pl.BlockSpec((None, ch, width), lambda c: (layer, c, 0)),
        ],
        out_specs=out_specs,
        out_shape=out_shape,
        scratch_shapes=scratch,
        compiler_params=pltpu.CompilerParams(
            vmem_limit_bytes=63 * 2**20, dimension_semantics=("arbitrary",)
        ),
        cost_estimate=pl.CostEstimate(
            flops=8 * rows * width * hidden,
            bytes_accessed=12 * width * hidden + 2 * rows * (3 * width + hidden),
            transcendentals=rows * hidden,
        ),
        name="bwd_block",
    )(g, x, a, w_up, w_down)


def update_body(with_weights, n_part, me_ref, lr_ref, decay_ref, gu_ref, *refs):
    refs = list(refs)
    width = gu_ref.shape[1]
    parts, refs = refs[:n_part], refs[n_part:]
    mu_ref, md_ref = refs[:2]
    refs = refs[2:]
    if with_weights:
        wu_ref, wd_ref = refs[:2]
        refs = refs[2:]
    refs = refs[2:]
    nmu_ref, nmd_ref = refs[:2]
    decay = decay_ref[0]
    mom = decay * mu_ref[...] + gu_ref[...].astype(F32)
    nmu_ref[...] = mom
    if with_weights:
        lr = lr_ref[0]
        refs[2][...] = wu_ref[...] - lr * mom
    for p, part in enumerate(parts):
        cols = slice(p * width, (p + 1) * width)
        mom = decay * md_ref[:, cols] + part[...].astype(F32)
        nmd_ref[:, cols] = mom
        if with_weights:
            refs[3][:, cols] = wd_ref[:, cols] - lr * mom


def update_shard(me, gsum, mom_up, mom_down, w_up, w_down, bufs, layer, learn_rate, mom_decay, with_weights):
    _, width, ch = mom_up.shape
    n_part = width // ch
    steps = 4
    rows_u, rows_d = width // steps, ch // steps
    smem = pl.BlockSpec(memory_space=pltpu.SMEM)
    any_spec = pl.BlockSpec(memory_space=pl.ANY)
    up_spec = pl.BlockSpec((None, rows_u, ch), lambda c, m: (layer, c, 0))
    down_spec = pl.BlockSpec((None, rows_d, width), lambda c, m: (layer, c, 0))
    in_specs = [smem, smem, pl.BlockSpec((rows_u, ch), lambda c, m: (c, 0))]
    args = [learn_rate, mom_decay, gsum]
    for p in range(n_part):
        first = (width + p * ch) // rows_d
        in_specs.append(pl.BlockSpec((rows_d, ch), lambda c, m, first=first: (first + c, 0)))
        args.append(gsum)
    in_specs += [up_spec, down_spec]
    args += [mom_up, mom_down]
    if with_weights:
        in_specs += [
            pl.BlockSpec((None, rows_u, ch), lambda c, m: (layer, c, m[0])),
            pl.BlockSpec((None, rows_d, width), lambda c, m: (layer, m[0] * steps + c, 0)),
        ]
        args += [w_up, w_down]
    in_specs += [any_spec, any_spec]
    args += list(bufs)
    out_specs = [up_spec, down_spec]
    out_shape = [jax.ShapeDtypeStruct(mom_up.shape, F32), jax.ShapeDtypeStruct(mom_down.shape, F32)]
    if with_weights:
        out_specs += [
            pl.BlockSpec((rows_u, ch), lambda c, m: (c, 0)),
            pl.BlockSpec((rows_d, width), lambda c, m: (c, 0)),
        ]
        out_shape += [jax.ShapeDtypeStruct((width, ch), F32), jax.ShapeDtypeStruct((ch, width), F32)]
    n_in = len(args) + 1
    return pl.pallas_call(
        functools.partial(update_body, with_weights, n_part),
        grid_spec=pltpu.PrefetchScalarGridSpec(
            num_scalar_prefetch=1, grid=(steps,), in_specs=in_specs, out_specs=out_specs
        ),
        out_shape=out_shape,
        input_output_aliases={n_in - 2: 0, n_in - 1: 1},
        compiler_params=pltpu.CompilerParams(
            vmem_limit_bytes=62 * 2**20, dimension_semantics=("arbitrary",)
        ),
        cost_estimate=pl.CostEstimate(
            flops=4_000_000_000, bytes_accessed=40 * width * ch, transcendentals=0
        ),
        name="update",
    )(me, *args)


def fwd_next_body(from_grad, n_chunk, order_ref, *refs):
    refs = list(refs)
    x_ref = refs.pop(0)
    if from_grad:
        lr_ref, decay_ref, wu_ref, wd_ref, m_ref = refs[:5]
        del refs[:5]
    up_parts = refs[:n_chunk]
    down_parts = refs[n_chunk:2 * n_chunk]
    del refs[:2 * n_chunk]
    del refs[:2]
    nwu_ref, nwd_ref, xo_ref, u_s, acc_s, pu_s, pd_s, sem = refs
    c = pl.program_id(0)
    last = n_chunk - 1
    rows, width = x_ref.shape
    rb = rows // ROW_BLOCKS
    ch = pu_s.shape[2]

    def start(j, slot):
        pltpu.make_async_copy(up_parts[j], pu_s.at[slot], sem.at[0, slot]).start()
        pltpu.make_async_copy(down_parts[j], pd_s.at[slot], sem.at[1, slot]).start()

    @pl.when(c == 0)
    def _():
        start(0, 0)

    for j in range(1, n_chunk):
        @pl.when(c + 1 == j)
        def _():
            start(j, j % 2)

    @pl.when(c == 0)
    def _():
        @pl.loop(0, ROW_BLOCKS)
        def _(r):
            rs = row_slice(r, rb)
            u_s[rs, :] = norm_rows(x_ref[rs, :].astype(F32)).astype(BF)
            acc_s[rs, :] = jnp.zeros((rb, width), F32)

    slot = lax.rem(c, 2)
    pltpu.make_async_copy(up_parts[0], pu_s.at[slot], sem.at[0, slot]).wait()
    pltpu.make_async_copy(down_parts[0], pd_s.at[slot], sem.at[1, slot]).wait()
    if from_grad:
        lr, decay = lr_ref[0], decay_ref[0]
        mom = decay * m_ref[0:width, :] + pu_s[slot].astype(F32)
        nwu_ref[...] = wu_ref[...] - lr * mom
        for part in range(width // ch):
            cols = slice(part * ch, (part + 1) * ch)
            m_rows = slice(width + part * ch, width + (part + 1) * ch)
            mom = decay * m_ref[m_rows, :] + pd_s[slot, :, cols].astype(F32)
            nwd_ref[:, cols] = wd_ref[:, cols] - lr * mom
    else:
        nwu_ref[...] = pu_s[slot]
        nwd_ref[...] = pd_s[slot]
    wu = nwu_ref[...].astype(BF)
    wd = nwd_ref[...].astype(BF)

    def up(r):
        a = jnp.dot(u_s[pl.ds(r * rb, rb), :], wu, preferred_element_type=F32).astype(BF)
        return gelu_tanh(a.astype(F32)).astype(BF)

    z = up(0)
    for r in range(ROW_BLOCKS):
        z_next = up(r + 1) if r + 1 < ROW_BLOCKS else None
        acc_s[pl.ds(r * rb, rb), :] += jnp.dot(z, wd, preferred_element_type=F32)
        z = z_next

    @pl.when(c == last)
    def _():
        @pl.loop(0, ROW_BLOCKS)
        def _(r):
            rs = row_slice(r, rb)
            y = acc_s[rs, :].astype(BF).astype(F32)
            xo_ref[rs, :] = (x_ref[rs, :].astype(F32) + y).astype(BF)


def fwd_next(order, x, up_parts, down_parts, bufs, layer, grad_args=None):
    rows, width = x.shape
    n_chunk = len(up_parts)
    ch = up_parts[0].shape[1]
    hidden = n_chunk * ch
    from_grad = grad_args is not None
    part_dtype = up_parts[0].dtype
    in_specs = [pl.BlockSpec((rows, width), lambda c, o: (0, 0), pipeline_mode=ONCE)]
    args = [x]
    up_spec = pl.BlockSpec((None, width, ch), lambda c, o: (layer, 0, o[c]))
    down_spec = pl.BlockSpec((None, ch, width), lambda c, o: (layer, o[c], 0))
    if from_grad:
        learn_rate, mom_decay, w_up, w_down, mom_all, mom_index = grad_args
        in_specs += [
            pl.BlockSpec(memory_space=pltpu.SMEM),
            pl.BlockSpec(memory_space=pltpu.SMEM),
            up_spec,
            down_spec,
            pl.BlockSpec((None, None, 2 * width, ch), lambda c, o: (o[c], mom_index, 0, 0)),
        ]
        args += [learn_rate, mom_decay, w_up, w_down, mom_all]
    any_spec = pl.BlockSpec(memory_space=pl.ANY)
    in_specs += [any_spec] * (2 * n_chunk + 2)
    args += list(up_parts) + list(down_parts) + list(bufs)
    n_in = len(args) + 1
    aliases = {n_in - 2: 0, n_in - 1: 1}
    return pl.pallas_call(
        functools.partial(fwd_next_body, from_grad, n_chunk),
        grid_spec=pltpu.PrefetchScalarGridSpec(
            num_scalar_prefetch=1,
            grid=(n_chunk,),
            in_specs=in_specs,
            out_specs=[
                up_spec,
                down_spec,
                pl.BlockSpec((rows, width), lambda c, o: (0, 0), pipeline_mode=ONCE),
            ],
            scratch_shapes=[
                pltpu.VMEM((rows, width), BF),
                pltpu.VMEM((rows, width), F32),
                pltpu.VMEM((2, width, ch), part_dtype),
                pltpu.VMEM((2, ch, width), part_dtype),
                pltpu.SemaphoreType.DMA((2, 2)),
            ],
        ),
        out_shape=[
            jax.ShapeDtypeStruct(bufs[0].shape, F32),
            jax.ShapeDtypeStruct(bufs[1].shape, F32),
            jax.ShapeDtypeStruct((rows, width), BF),
        ],
        input_output_aliases=aliases,
        compiler_params=pltpu.CompilerParams(
            vmem_limit_bytes=63 * 2**20, dimension_semantics=("arbitrary",)
        ),
        cost_estimate=pl.CostEstimate(
            flops=4 * rows * width * hidden,
            bytes_accessed=24 * width * hidden,
            transcendentals=rows * hidden,
        ),
        name="fwd_next",
    )(order, *args)


def alloc_body(up_ref, down_ref):
    pass


def alloc(up_shape, down_shape):
    any_spec = pl.BlockSpec(memory_space=pl.ANY)
    return pl.pallas_call(
        alloc_body,
        out_specs=[any_spec, any_spec],
        out_shape=[jax.ShapeDtypeStruct(up_shape, F32), jax.ShapeDtypeStruct(down_shape, F32)],
        compiler_params=pltpu.CompilerParams(has_side_effects=False),
        name="alloc",
    )()


def gather_pair(first, second, n_dev):
    def swap(block, bit):
        return lax.ppermute(block, "data", [(i, i ^ bit) for i in range(n_dev)])

    f2 = swap(first, 2)
    s4 = swap(second, 4)
    f4, f6 = swap(first, 4), swap(f2, 4)
    s2, s6 = swap(second, 2), swap(s4, 2)
    firsts = {0: first, 2: f2, 4: f4, 6: f6}
    seconds = {0: second, 2: s2, 4: s4, 6: s6}
    for j in (0, 2, 4, 6):
        firsts[j + 1] = swap(firsts[j], 1)
        seconds[j + 1] = swap(seconds[j], 1)
    return [firsts[j] for j in range(n_dev)], [seconds[j] for j in range(n_dev)]


def solution(mesh):
    n_dev = mesh.shape["data"]

    def local_step(x_now, x_next, labels, w_up, w_down, w_head, mom_up, mom_down, mom_head, learn_rate, mom_decay):
        n_img, n_tok, width = x_now.shape
        layers, _, hidden = w_up.shape
        ch = hidden // n_dev
        batch_total = n_img * n_dev
        n_rows = n_img * n_tok
        rows = -(-n_rows // (16 * ROW_BLOCKS)) * (16 * ROW_BLOCKS)
        me = lax.axis_index("data")
        order = jnp.bitwise_xor(me, jnp.arange(n_dev, dtype=jnp.int32)).astype(jnp.int32)

        def pad_rows(x):
            return jnp.pad(x.reshape(n_rows, width), ((0, rows - n_rows), (0, 0)))

        row_id = lax.broadcasted_iota(jnp.int32, (n_img, rows), 1)
        img_id = lax.broadcasted_iota(jnp.int32, (n_img, rows), 0)
        member = ((row_id >= img_id * n_tok) & (row_id < (img_id + 1) * n_tok)).astype(BF)

        def down_split(m):
            return jnp.concatenate([m[..., p * ch:(p + 1) * ch] for p in range(width // ch)], axis=-2)

        def down_join(m):
            return jnp.concatenate([m[p * ch:(p + 1) * ch] for p in range(width // ch)], axis=1)

        mom_pack = jnp.concatenate([mom_up[:EARLY], down_split(mom_down[:EARLY])], axis=1)
        mom_head_all = lax.all_gather(mom_head, "data", axis=0, tiled=True)
        mom_all = lax.all_gather(mom_pack, "data", axis=0)

        def head(rows_x, head_b):
            sums = jnp.dot(member, rows_x, preferred_element_type=F32)
            pooled = sums / n_tok
            normed = norm_rows(pooled).astype(BF)
            return jnp.dot(normed, head_b, preferred_element_type=F32), pooled, normed

        x0 = pad_rows(x_now)
        pre_acts, outs = fwd_now(x0, w_up, w_down, n_dev)
        head_b = w_head.astype(BF)
        logits, pooled, normed = head(outs[layers - 1], head_b)
        soft_probs = jax.nn.softmax(logits, axis=-1)
        targets = jax.nn.one_hot(labels, logits.shape[-1], dtype=F32)
        grad_logits = ((soft_probs - targets) / batch_total).astype(BF)
        grad_normed = lax.dot_general(grad_logits, head_b, CONTRACT_LAST, preferred_element_type=F32).astype(BF)
        _, norm_pull = jax.vjp(norm_rows, pooled)
        grad_pooled = norm_pull(grad_normed.astype(F32))[0]
        grad_img = (grad_pooled / n_tok).astype(BF)
        g = lax.dot_general(member, grad_img, CONTRACT_ROWS, preferred_element_type=F32).astype(BF)

        classes = logits.shape[-1]
        factors = jnp.concatenate([normed, jnp.pad(grad_logits, ((0, 0), (0, -classes % 128)))], axis=1)
        factors = lax.all_gather(factors, "data", axis=0)
        g, factors = lax.optimization_barrier((g, factors))
        head_sum = jnp.zeros(w_head.shape, F32)
        for i in range(n_dev):
            term = lax.dot_general(
                factors[i, :, :width], factors[i, :, width:width + classes], CONTRACT_ROWS,
                preferred_element_type=F32,
            )
            head_sum = head_sum + term.astype(BF).astype(F32)
        head_sum = head_sum.astype(BF).astype(F32)
        whole_mom_head = mom_decay * mom_head_all + head_sum
        head_width = mom_head.shape[0]
        new_mom_head = lax.dynamic_slice_in_dim(whole_mom_head, me * head_width, head_width, axis=0)
        new_w_head = w_head - learn_rate * whole_mom_head

        parts = [None] * layers
        mom_bufs = alloc(mom_up.shape, mom_down.shape)
        me1, lr1, decay1 = me.reshape(1), learn_rate.reshape(1), mom_decay.reshape(1)
        for layer in reversed(range(layers)):
            x_in = (outs, layer - 1) if layer > 0 else (x0, 0)
            res = bwd_block(g, x_in[0], x_in[1], pre_acts, w_up, w_down, layer, n_dev)
            dw = res[0]
            g = res[1] if layer > 0 else None
            gsum = lax.psum_scatter(dw, "data", scatter_dimension=0, tiled=True)[0]
            early = layer < EARLY
            res = update_shard(me1, gsum, mom_up, mom_down, w_up, w_down, mom_bufs, layer, lr1, decay1, not early)
            mom_bufs = res[:2]
            if early:
                cut = [gsum[:width], down_join(gsum[width:])]
            else:
                cut = res[2:]
            parts[layer] = gather_pair(cut[0], cut[1], n_dev)

        new_mom_up, new_mom_down = mom_bufs
        bufs = alloc(w_up.shape, w_down.shape)
        x = pad_rows(x_next)
        for layer in range(layers):
            grad_args = None
            if layer < EARLY:
                grad_args = (lr1, decay1, w_up, w_down, mom_all, layer)
            *bufs, x = fwd_next(order, x, parts[layer][0], parts[layer][1], bufs, layer, grad_args)
        new_w_up, new_w_down = bufs
        logits_next = head(x, new_w_head.astype(BF))[0]
        return (logits_next, new_w_up, new_w_down, new_w_head, new_mom_up, new_mom_down, new_mom_head)

    spec_up = P(None, None, "data")
    spec_down = P(None, "data", None)
    spec_head = P("data", None)

    return jax.shard_map(
        local_step,
        mesh=mesh,
        in_specs=(P("data"), P("data"), P("data"), P(), P(), P(), spec_up, spec_down, spec_head, P(), P()),
        out_specs=(P("data"), P(), P(), P(), spec_up, spec_down, spec_head),
        check_vma=False,
    )
```

```python
import functools

import jax
import jax.numpy as jnp
from jax import lax
from jax.experimental import pallas as pl
from jax.experimental.pallas import tpu as pltpu
from jax.sharding import PartitionSpec as P


LN_EPS = 1e-6
GELU_A = 0.7978845608028654
GELU_B = GELU_A * 0.044715
BF = jnp.bfloat16
F32 = jnp.float32
CONTRACT_ROWS = (((0,), (0,)), ((), ()))
CONTRACT_LAST = (((1,), (1,)), ((), ()))
ONCE = pl.Buffered(1)
ROW_BLOCKS = 5
EARLY = 3
EARLY_SC = 3


def norm_rows(values):
    mean_v = jnp.mean(values, axis=-1, keepdims=True)
    centered = values - mean_v
    var_v = jnp.mean(centered * centered, axis=-1, keepdims=True)
    return centered * lax.rsqrt(var_v + LN_EPS)


def gelu_tanh(a):
    t = jnp.tanh(a * (GELU_A + GELU_B * (a * a)))
    return a * (0.5 + 0.5 * t)


def row_slice(r, size):
    return pl.ds(pl.multiple_of(r * size, 16), size)


def fwd_now_body(x_ref, wu_ref, wd_ref, a_ref, xo_ref, x_s, u_s, acc_s):
    layer, c = pl.program_id(0), pl.program_id(1)
    last = pl.num_programs(1) - 1
    rb = x_s.shape[0] // ROW_BLOCKS

    @pl.when((layer == 0) & (c == 0))
    def _():
        @pl.loop(0, ROW_BLOCKS)
        def _(r):
            rs = row_slice(r, rb)
            x = x_ref[rs, :]
            x_s[rs, :] = x
            u_s[rs, :] = norm_rows(x.astype(F32)).astype(BF)
            acc_s[rs, :] = jnp.zeros((rb, x.shape[1]), F32)

    wu = wu_ref[...].astype(BF)
    wd = wd_ref[...].astype(BF)

    def up(r):
        rs = pl.ds(r * rb, rb)
        a = jnp.dot(u_s[rs, :], wu, preferred_element_type=F32).astype(BF)
        a_ref[rs, :] = a
        return gelu_tanh(a.astype(F32)).astype(BF)

    z = up(0)
    for r in range(ROW_BLOCKS):
        z_next = up(r + 1) if r + 1 < ROW_BLOCKS else None
        acc_s[pl.ds(r * rb, rb), :] += jnp.dot(z, wd, preferred_element_type=F32)
        z = z_next

    @pl.when(c == last)
    def _():
        @pl.loop(0, ROW_BLOCKS)
        def _(r):
            rs = row_slice(r, rb)
            x = (x_s[rs, :].astype(F32) + acc_s[rs, :].astype(BF).astype(F32)).astype(BF)
            x_s[rs, :] = x
            xo_ref[rs, :] = x
            u_s[rs, :] = norm_rows(x.astype(F32)).astype(BF)
            acc_s[rs, :] = jnp.zeros((rb, x.shape[1]), F32)


def fwd_now(x, w_up, w_down, n_chunk):
    rows, width = x.shape
    layers, _, hidden = w_up.shape
    ch = hidden // n_chunk
    return pl.pallas_call(
        fwd_now_body,
        grid=(layers, n_chunk),
        in_specs=[
            pl.BlockSpec((rows, width), lambda l, c: (0, 0), pipeline_mode=ONCE),
            pl.BlockSpec((None, width, ch), lambda l, c: (l, 0, c)),
            pl.BlockSpec((None, ch, width), lambda l, c: (l, c, 0)),
        ],
        out_specs=[
            pl.BlockSpec((None, rows, ch), lambda l, c: (l, 0, c)),
            pl.BlockSpec((None, rows, width), lambda l, c: (l, 0, 0)),
        ],
        out_shape=[
            jax.ShapeDtypeStruct((layers, rows, hidden), BF),
            jax.ShapeDtypeStruct((layers, rows, width), BF),
        ],
        scratch_shapes=[
            pltpu.VMEM((rows, width), BF),
            pltpu.VMEM((rows, width), BF),
            pltpu.VMEM((rows, width), F32),
        ],
        compiler_params=pltpu.CompilerParams(
            vmem_limit_bytes=62 * 2**20, dimension_semantics=("arbitrary", "arbitrary")
        ),
        cost_estimate=pl.CostEstimate(
            flops=layers * 4 * rows * width * hidden,
            bytes_accessed=layers * (8 * width * hidden + 2 * rows * (width + hidden)),
            transcendentals=layers * rows * hidden,
        ),
        name="fwd_now",
    )(x, w_up, w_down)


def bwd_body(need_dx, g_ref, x_ref, a_ref, wu_ref, wd_ref, dw_ref, *rest):
    if need_dx:
        go_ref, u_s, z_s, dp_s, acc_s = rest
    else:
        u_s, z_s, dp_s = rest
    c = pl.program_id(0)
    last = pl.num_programs(0) - 1
    rb = u_s.shape[0] // ROW_BLOCKS
    width = u_s.shape[1]
    ch = z_s.shape[1]

    @pl.when(c == 0)
    def _():
        @pl.loop(0, ROW_BLOCKS)
        def _(r):
            rs = row_slice(r, rb)
            u_s[rs, :] = norm_rows(x_ref[rs, :].astype(F32)).astype(BF)
            if need_dx:
                acc_s[rs, :] = jnp.zeros((rb, width), F32)

    wd = wd_ref[...].astype(BF)
    wu = wu_ref[...].astype(BF) if need_dx else None

    def grad_pre(r):
        rs = pl.ds(r * rb, rb)
        dz = lax.dot_general(g_ref[rs, :], wd, CONTRACT_LAST, preferred_element_type=F32)
        dz = dz.astype(BF).astype(F32)
        a = a_ref[rs, :].astype(F32)
        a2 = a * a
        t = jnp.tanh(a * (GELU_A + GELU_B * a2))
        s = 0.5 + 0.5 * t
        z = a * s
        slope = s + (z * (0.5 - 0.5 * t)) * (2 * GELU_A + (6 * GELU_B) * a2)
        dp = (slope * dz).astype(BF)
        z_s[rs, :] = z.astype(BF)
        dp_s[rs, :] = dp
        return dp

    dp = grad_pre(0)
    for r in range(ROW_BLOCKS):
        dp_next = grad_pre(r + 1) if r + 1 < ROW_BLOCKS else None
        if need_dx:
            du = lax.dot_general(dp, wu, CONTRACT_LAST, preferred_element_type=F32)
            acc_s[pl.ds(r * rb, rb), :] += du
        dp = dp_next

    dwd = lax.dot_general(z_s[...], g_ref[...], CONTRACT_ROWS, preferred_element_type=F32)
    dwd = dwd.astype(BF)
    dwu = lax.dot_general(u_s[...], dp_s[...], CONTRACT_ROWS, preferred_element_type=F32)
    dw_ref[0:width, :] = dwu.astype(BF)
    for part in range(width // ch):
        dw_ref[width + part * ch:width + (part + 1) * ch, :] = dwd[:, part * ch:(part + 1) * ch]

    if need_dx:
        @pl.when(c == last)
        def _():
            @pl.loop(0, ROW_BLOCKS)
            def _(r):
                rs = row_slice(r, rb)
                xw = x_ref[rs, :].astype(F32)
                centered = xw - jnp.mean(xw, axis=-1, keepdims=True)
                var_v = jnp.mean(centered * centered, axis=-1, keepdims=True)
                rstd = lax.rsqrt(var_v + LN_EPS)
                xhat = centered * rstd
                du = acc_s[rs, :].astype(BF).astype(F32)
                m1 = jnp.mean(du, axis=-1, keepdims=True)
                m2 = jnp.mean(du * xhat, axis=-1, keepdims=True)
                dx = rstd * (du - m1 - xhat * m2)
                go_ref[rs, :] = (g_ref[rs, :].astype(F32) + dx).astype(BF)


def bwd_block(g, x, x_index, a, w_up, w_down, layer, n_chunk):
    rows, width = g.shape
    hidden = w_up.shape[2]
    ch = hidden // n_chunk
    need_dx = layer > 0
    if x.ndim == 3:
        x_spec = pl.BlockSpec((None, rows, width), lambda c: (x_index, 0, 0), pipeline_mode=ONCE)
    else:
        x_spec = pl.BlockSpec((rows, width), lambda c: (0, 0), pipeline_mode=ONCE)
    dw_rows = 2 * width
    out_specs = [pl.BlockSpec((None, dw_rows, ch), lambda c: (c, 0, 0))]
    out_shape = [jax.ShapeDtypeStruct((n_chunk, dw_rows, ch), BF)]
    scratch = [pltpu.VMEM((rows, width), BF), pltpu.VMEM((rows, ch), BF), pltpu.VMEM((rows, ch), BF)]
    if need_dx:
        out_specs.append(pl.BlockSpec((rows, width), lambda c: (0, 0), pipeline_mode=ONCE))
        out_shape.append(jax.ShapeDtypeStruct((rows, width), BF))
        scratch.append(pltpu.VMEM((rows, width), F32))
    return pl.pallas_call(
        functools.partial(bwd_body, need_dx),
        grid=(n_chunk,),
        in_specs=[
            pl.BlockSpec((rows, width), lambda c: (0, 0), pipeline_mode=ONCE),
            x_spec,
            pl.BlockSpec((None, rows, ch), lambda c: (layer, 0, c)),
            pl.BlockSpec((None, width, ch), lambda c: (layer, 0, c)),
            pl.BlockSpec((None, ch, width), lambda c: (layer, c, 0)),
        ],
        out_specs=out_specs,
        out_shape=out_shape,
        scratch_shapes=scratch,
        compiler_params=pltpu.CompilerParams(
            vmem_limit_bytes=63 * 2**20, dimension_semantics=("arbitrary",)
        ),
        cost_estimate=pl.CostEstimate(
            flops=8 * rows * width * hidden,
            bytes_accessed=12 * width * hidden + 2 * rows * (3 * width + hidden),
            transcendentals=rows * hidden,
        ),
        name="bwd_block",
    )(g, x, a, w_up, w_down)


def update_body(with_weights, n_part, me_ref, lr_ref, decay_ref, gu_ref, *refs):
    refs = list(refs)
    width = gu_ref.shape[1]
    parts, refs = refs[:n_part], refs[n_part:]
    mu_ref, md_ref = refs[:2]
    refs = refs[2:]
    if with_weights:
        wu_ref, wd_ref = refs[:2]
        refs = refs[2:]
    refs = refs[2:]
    nmu_ref, nmd_ref = refs[:2]
    decay = decay_ref[0]
    mom = decay * mu_ref[...] + gu_ref[...].astype(F32)
    nmu_ref[...] = mom
    if with_weights:
        lr = lr_ref[0]
        refs[2][...] = wu_ref[...] - lr * mom
    for p, part in enumerate(parts):
        cols = slice(p * width, (p + 1) * width)
        mom = decay * md_ref[:, cols] + part[...].astype(F32)
        nmd_ref[:, cols] = mom
        if with_weights:
            refs[3][:, cols] = wd_ref[:, cols] - lr * mom


def update_shard(me, gsum, mom_up, mom_down, w_up, w_down, bufs, layer, learn_rate, mom_decay, with_weights):
    _, width, ch = mom_up.shape
    n_part = width // ch
    steps = 4
    rows_u, rows_d = width // steps, ch // steps
    smem = pl.BlockSpec(memory_space=pltpu.SMEM)
    any_spec = pl.BlockSpec(memory_space=pl.ANY)
    up_spec = pl.BlockSpec((None, rows_u, ch), lambda c, m: (layer, c, 0))
    down_spec = pl.BlockSpec((None, rows_d, width), lambda c, m: (layer, c, 0))
    in_specs = [smem, smem, pl.BlockSpec((rows_u, ch), lambda c, m: (c, 0))]
    args = [learn_rate, mom_decay, gsum]
    for p in range(n_part):
        first = (width + p * ch) // rows_d
        in_specs.append(pl.BlockSpec((rows_d, ch), lambda c, m, first=first: (first + c, 0)))
        args.append(gsum)
    in_specs += [up_spec, down_spec]
    args += [mom_up, mom_down]
    if with_weights:
        in_specs += [
            pl.BlockSpec((None, rows_u, ch), lambda c, m: (layer, c, m[0])),
            pl.BlockSpec((None, rows_d, width), lambda c, m: (layer, m[0] * steps + c, 0)),
        ]
        args += [w_up, w_down]
    in_specs += [any_spec, any_spec]
    args += list(bufs)
    out_specs = [up_spec, down_spec]
    out_shape = [jax.ShapeDtypeStruct(mom_up.shape, F32), jax.ShapeDtypeStruct(mom_down.shape, F32)]
    if with_weights:
        out_specs += [
            pl.BlockSpec((rows_u, ch), lambda c, m: (c, 0)),
            pl.BlockSpec((rows_d, width), lambda c, m: (c, 0)),
        ]
        out_shape += [jax.ShapeDtypeStruct((width, ch), F32), jax.ShapeDtypeStruct((ch, width), F32)]
    n_in = len(args) + 1
    return pl.pallas_call(
        functools.partial(update_body, with_weights, n_part),
        grid_spec=pltpu.PrefetchScalarGridSpec(
            num_scalar_prefetch=1, grid=(steps,), in_specs=in_specs, out_specs=out_specs
        ),
        out_shape=out_shape,
        input_output_aliases={n_in - 2: 0, n_in - 1: 1},
        compiler_params=pltpu.CompilerParams(
            vmem_limit_bytes=62 * 2**20, dimension_semantics=("arbitrary",)
        ),
        cost_estimate=pl.CostEstimate(
            flops=4_000_000_000, bytes_accessed=40 * width * ch, transcendentals=0
        ),
        name="update",
    )(me, *args)


def fwd_next_body(from_grad, mom_in_parts, n_chunk, order_ref, *refs):
    refs = list(refs)
    x_ref = refs.pop(0)
    if from_grad:
        lr_ref, decay_ref, wu_ref, wd_ref = refs[:4]
        del refs[:4]
        if mom_in_parts:
            mu_parts, md_parts = refs[:n_chunk], refs[n_chunk:2 * n_chunk]
            del refs[:2 * n_chunk]
        else:
            m_ref = refs.pop(0)
    up_parts = refs[:n_chunk]
    down_parts = refs[n_chunk:2 * n_chunk]
    del refs[:2 * n_chunk]
    del refs[:2]
    nwu_ref, nwd_ref, xo_ref, u_s, acc_s, pu_s, pd_s, sem = refs[:8]
    if mom_in_parts:
        mu_s, md_s = refs[8:]
    c = pl.program_id(0)
    last = n_chunk - 1
    rows, width = x_ref.shape
    rb = rows // ROW_BLOCKS
    ch = pu_s.shape[2]

    def copies(j, slot):
        pairs = [(up_parts[j], pu_s), (down_parts[j], pd_s)]
        if mom_in_parts:
            pairs += [(mu_parts[j], mu_s), (md_parts[j], md_s)]
        return [
            pltpu.make_async_copy(src, dst.at[slot], sem.at[i, slot]) for i, (src, dst) in enumerate(pairs)
        ]

    def start(j, slot):
        for copy in copies(j, slot):
            copy.start()

    @pl.when(c == 0)
    def _():
        start(0, 0)

    for j in range(1, n_chunk):
        @pl.when(c + 1 == j)
        def _():
            start(j, j % 2)

    @pl.when(c == 0)
    def _():
        @pl.loop(0, ROW_BLOCKS)
        def _(r):
            rs = row_slice(r, rb)
            u_s[rs, :] = norm_rows(x_ref[rs, :].astype(F32)).astype(BF)
            acc_s[rs, :] = jnp.zeros((rb, width), F32)

    slot = lax.rem(c, 2)
    for copy in copies(0, slot):
        copy.wait()
    if from_grad:
        lr, decay = lr_ref[0], decay_ref[0]
        m_up = mu_s[slot] if mom_in_parts else m_ref[0:width, :]
        mom = decay * m_up + pu_s[slot].astype(F32)
        nwu_ref[...] = wu_ref[...] - lr * mom
        for part in range(width // ch):
            cols = slice(part * ch, (part + 1) * ch)
            m_rows = slice(width + part * ch, width + (part + 1) * ch)
            m_down = md_s[slot, :, cols] if mom_in_parts else m_ref[m_rows, :]
            mom = decay * m_down + pd_s[slot, :, cols].astype(F32)
            nwd_ref[:, cols] = wd_ref[:, cols] - lr * mom
    else:
        nwu_ref[...] = pu_s[slot]
        nwd_ref[...] = pd_s[slot]
    wu = nwu_ref[...].astype(BF)
    wd = nwd_ref[...].astype(BF)

    def up(r):
        a = jnp.dot(u_s[pl.ds(r * rb, rb), :], wu, preferred_element_type=F32).astype(BF)
        return gelu_tanh(a.astype(F32)).astype(BF)

    z = up(0)
    for r in range(ROW_BLOCKS):
        z_next = up(r + 1) if r + 1 < ROW_BLOCKS else None
        acc_s[pl.ds(r * rb, rb), :] += jnp.dot(z, wd, preferred_element_type=F32)
        z = z_next

    @pl.when(c == last)
    def _():
        @pl.loop(0, ROW_BLOCKS)
        def _(r):
            rs = row_slice(r, rb)
            y = acc_s[rs, :].astype(BF).astype(F32)
            xo_ref[rs, :] = (x_ref[rs, :].astype(F32) + y).astype(BF)


def fwd_next(order, x, up_parts, down_parts, bufs, layer, grad_args=None):
    rows, width = x.shape
    n_chunk = len(up_parts)
    ch = up_parts[0].shape[1]
    hidden = n_chunk * ch
    from_grad = grad_args is not None
    mom_in_parts = from_grad and isinstance(grad_args[4], tuple)
    part_dtype = up_parts[0].dtype
    in_specs = [pl.BlockSpec((rows, width), lambda c, o: (0, 0), pipeline_mode=ONCE)]
    args = [x]
    up_spec = pl.BlockSpec((None, width, ch), lambda c, o: (layer, 0, o[c]))
    down_spec = pl.BlockSpec((None, ch, width), lambda c, o: (layer, o[c], 0))
    if from_grad:
        learn_rate, mom_decay, w_up, w_down, moms, mom_index = grad_args
        in_specs += [
            pl.BlockSpec(memory_space=pltpu.SMEM),
            pl.BlockSpec(memory_space=pltpu.SMEM),
            up_spec,
            down_spec,
        ]
        args += [learn_rate, mom_decay, w_up, w_down]
    any_spec = pl.BlockSpec(memory_space=pl.ANY)
    if mom_in_parts:
        in_specs += [any_spec] * (2 * n_chunk)
        args += list(moms[0]) + list(moms[1])
    elif from_grad:
        in_specs.append(pl.BlockSpec((None, None, 2 * width, ch), lambda c, o: (o[c], mom_index, 0, 0)))
        args.append(moms)
    in_specs += [any_spec] * (2 * n_chunk + 2)
    args += list(up_parts) + list(down_parts) + list(bufs)
    n_in = len(args) + 1
    aliases = {n_in - 2: 0, n_in - 1: 1}
    mom_scratch = []
    if mom_in_parts:
        mom_scratch = [pltpu.VMEM((2, width, ch), F32), pltpu.VMEM((2, ch, width), F32)]
    return pl.pallas_call(
        functools.partial(fwd_next_body, from_grad, mom_in_parts, n_chunk),
        grid_spec=pltpu.PrefetchScalarGridSpec(
            num_scalar_prefetch=1,
            grid=(n_chunk,),
            in_specs=in_specs,
            out_specs=[
                up_spec,
                down_spec,
                pl.BlockSpec((rows, width), lambda c, o: (0, 0), pipeline_mode=ONCE),
            ],
            scratch_shapes=[
                pltpu.VMEM((rows, width), BF),
                pltpu.VMEM((rows, width), F32),
                pltpu.VMEM((2, width, ch), part_dtype),
                pltpu.VMEM((2, ch, width), part_dtype),
                pltpu.SemaphoreType.DMA((4, 2)),
                *mom_scratch,
            ],
        ),
        out_shape=[
            jax.ShapeDtypeStruct(bufs[0].shape, F32),
            jax.ShapeDtypeStruct(bufs[1].shape, F32),
            jax.ShapeDtypeStruct((rows, width), BF),
        ],
        input_output_aliases=aliases,
        compiler_params=pltpu.CompilerParams(
            vmem_limit_bytes=63 * 2**20, dimension_semantics=("arbitrary",)
        ),
        cost_estimate=pl.CostEstimate(
            flops=4 * rows * width * hidden,
            bytes_accessed=24 * width * hidden,
            transcendentals=rows * hidden,
        ),
        name="fwd_next",
    )(order, *args)


def alloc_body(up_ref, down_ref):
    pass


def alloc(up_shape, down_shape):
    any_spec = pl.BlockSpec(memory_space=pl.ANY)
    return pl.pallas_call(
        alloc_body,
        out_specs=[any_spec, any_spec],
        out_shape=[jax.ShapeDtypeStruct(up_shape, F32), jax.ShapeDtypeStruct(down_shape, F32)],
        compiler_params=pltpu.CompilerParams(has_side_effects=False),
        name="alloc",
    )()


def gather_pair(first, second, n_dev):
    def swap(block, bit):
        return lax.ppermute(block, "data", [(i, i ^ bit) for i in range(n_dev)])

    f2 = swap(first, 2)
    s4 = swap(second, 4)
    f4, s2 = swap(first, 4), swap(second, 2)
    f6, s6 = swap(f2, 4), swap(s4, 2)
    firsts = {0: first, 2: f2, 4: f4, 6: f6}
    seconds = {0: second, 2: s2, 4: s4, 6: s6}
    for j in (0, 2, 4, 6):
        firsts[j + 1] = swap(firsts[j], 1)
        seconds[j + 1] = swap(seconds[j], 1)
    return tuple(firsts[j] for j in range(n_dev)), tuple(seconds[j] for j in range(n_dev))


def solution(mesh):
    n_dev = mesh.shape["data"]

    def local_step(x_now, x_next, labels, w_up, w_down, w_head, mom_up, mom_down, mom_head, learn_rate, mom_decay):
        n_img, n_tok, width = x_now.shape
        layers, _, hidden = w_up.shape
        ch = hidden // n_dev
        batch_total = n_img * n_dev
        n_rows = n_img * n_tok
        rows = -(-n_rows // (16 * ROW_BLOCKS)) * (16 * ROW_BLOCKS)
        me = lax.axis_index("data")
        order = jnp.bitwise_xor(me, jnp.arange(n_dev, dtype=jnp.int32)).astype(jnp.int32)

        slot_of = ((order >> 1) & 1) + 2 * ((order >> 2) & 1) + 4 * (order & 1)

        def pad_rows(x):
            return jnp.pad(x.reshape(n_rows, width), ((0, rows - n_rows), (0, 0)))

        row_id = lax.broadcasted_iota(jnp.int32, (n_img, rows), 1)
        img_id = lax.broadcasted_iota(jnp.int32, (n_img, rows), 0)
        member = ((row_id >= img_id * n_tok) & (row_id < (img_id + 1) * n_tok)).astype(BF)

        def down_split(m):
            return jnp.concatenate([m[..., p * ch:(p + 1) * ch] for p in range(width // ch)], axis=-2)

        def down_join(m):
            return jnp.concatenate([m[p * ch:(p + 1) * ch] for p in range(width // ch)], axis=1)

        mom_pack = jnp.concatenate([mom_up[:EARLY_SC], down_split(mom_down[:EARLY_SC])], axis=1)

        def gather_small(block):
            for bit in (2, 4, 1):
                other = lax.ppermute(block, "data", [(i, i ^ bit) for i in range(n_dev)])
                block = jnp.concatenate([block, other], axis=0)
            return jnp.take(block, slot_of, axis=0)

        mom_all = lax.all_gather(mom_pack, "data", axis=0)

        def head(rows_x, head_b):
            sums = jnp.dot(member, rows_x, preferred_element_type=F32)
            pooled = sums / n_tok
            normed = norm_rows(pooled).astype(BF)
            return jnp.dot(normed, head_b, preferred_element_type=F32), pooled, normed

        x0 = pad_rows(x_now)
        pre_acts, outs = fwd_now(x0, w_up, w_down, n_dev)
        head_b = w_head.astype(BF)
        logits, pooled, normed = head(outs[layers - 1], head_b)
        soft_probs = jax.nn.softmax(logits, axis=-1)
        targets = jax.nn.one_hot(labels, logits.shape[-1], dtype=F32)
        grad_logits = ((soft_probs - targets) / batch_total).astype(BF)
        grad_normed = lax.dot_general(grad_logits, head_b, CONTRACT_LAST, preferred_element_type=F32).astype(BF)
        _, norm_pull = jax.vjp(norm_rows, pooled)
        grad_pooled = norm_pull(grad_normed.astype(F32))[0]
        grad_img = (grad_pooled / n_tok).astype(BF)
        g = lax.dot_general(member, grad_img, CONTRACT_ROWS, preferred_element_type=F32).astype(BF)

        classes = logits.shape[-1]
        factors = jnp.concatenate([normed, jnp.pad(grad_logits, ((0, 0), (0, -classes % 128)))], axis=1)
        factors = gather_small(factors[None])
        mom_head_all = gather_small(mom_head[None]).reshape(w_head.shape)
        head_sum = jnp.zeros(w_head.shape, F32)
        for i in range(n_dev):
            term = lax.dot_general(
                factors[i, :, :width], factors[i, :, width:width + classes], CONTRACT_ROWS,
                preferred_element_type=F32,
            )
            head_sum = head_sum + term.astype(BF).astype(F32)
        head_sum = head_sum.astype(BF).astype(F32)
        whole_mom_head = mom_decay * mom_head_all + head_sum
        head_width = mom_head.shape[0]
        new_mom_head = lax.dynamic_slice_in_dim(whole_mom_head, me * head_width, head_width, axis=0)
        new_w_head = w_head - learn_rate * whole_mom_head

        mom_parts = {l: gather_pair(mom_up[l], mom_down[l], n_dev) for l in range(EARLY_SC, EARLY)}
        parts = [None] * layers
        mom_bufs = alloc(mom_up.shape, mom_down.shape)
        me1, lr1, decay1 = me.reshape(1), learn_rate.reshape(1), mom_decay.reshape(1)
        for layer in reversed(range(layers)):
            x_in = (outs, layer - 1) if layer > 0 else (x0, 0)
            res = bwd_block(g, x_in[0], x_in[1], pre_acts, w_up, w_down, layer, n_dev)
            dw = res[0]
            g = res[1] if layer > 0 else None
            if layer == 2:
                g, x_next = lax.optimization_barrier((g, x_next))
                x_pad = pad_rows(x_next)
            if layer == 1:
                g, new_w_head, new_mom_head, x_pad = lax.optimization_barrier((g, new_w_head, new_mom_head, x_pad))
            gsum = lax.psum_scatter(dw, "data", scatter_dimension=0, tiled=True)[0]
            early = layer < EARLY
            res = update_shard(me1, gsum, mom_up, mom_down, w_up, w_down, mom_bufs, layer, lr1, decay1, not early)
            mom_bufs = res[:2]
            if early:
                cut = [gsum[:width], down_join(gsum[width:])]
            else:
                cut = res[2:]
            parts[layer] = gather_pair(cut[0], cut[1], n_dev)

        new_mom_up, new_mom_down = mom_bufs
        bufs = alloc(w_up.shape, w_down.shape)
        x = x_pad
        for layer in range(layers):
            grad_args = None
            if layer < EARLY:
                moms = mom_all if layer < EARLY_SC else mom_parts[layer]
                grad_args = (lr1, decay1, w_up, w_down, moms, layer)
            *bufs, x = fwd_next(order, x, parts[layer][0], parts[layer][1], bufs, layer, grad_args)
        new_w_up, new_w_down = bufs
        logits_next = head(x, new_w_head.astype(BF))[0]
        return (logits_next, new_w_up, new_w_down, new_w_head, new_mom_up, new_mom_down, new_mom_head)

    spec_up = P(None, None, "data")
    spec_down = P(None, "data", None)
    spec_head = P("data", None)

    return jax.shard_map(
        local_step,
        mesh=mesh,
        in_specs=(P("data"), P("data"), P("data"), P(), P(), P(), spec_up, spec_down, spec_head, P(), P()),
        out_specs=(P("data"), P(), P(), P(), spec_up, spec_down, spec_head),
        check_vma=False,
    )
```
